32 devices in a mesh: ez: 4 (over z), ey: 2 (over y), ex: 4 (over x, core).
Axes of the slice: x: 2, y: 2, z: 4, core: 2. Of those that a mesh axis runs over, the one named last changes fastest.
Arguments:
- tokens_in: bfloat16 [2, 8192, 1024], P(None, ('ez', 'ey', 'ex'))
- expert_ids: int32 [2, 2, 8192, 2], P(None, None, ('ez', 'ey', 'ex'))
- gate_vals: float32 [2, 2, 8192, 2], P(None, None, ('ez', 'ey', 'ex'))
- w_up1: bfloat16 [2, 32, 1024, 2816], P(None, ('ez', 'ey', 'ex'))
- w_up3: bfloat16 [2, 32, 1024, 2816], P(None, ('ez', 'ey', 'ex'))
- w_down: bfloat16 [2, 32, 2816, 1024], P(None, ('ez', 'ey', 'ex'))
Outputs:
- output: bfloat16 [2, 8192, 1024], P(None, ('ez', 'ey', 'ex'))
All inputs are finite; a program needn't handle non-finite values.
Results may differ from the reference program's by a relative error of at most 0.0151252.
Values are sent between devices in bfloat16 or wider.
A program may use at most 1 GiB of HBM per device.

```python
import jax
import jax.numpy as jnp
import numpy as np
from jax import lax

HIDDEN = 1024
FFN_DIM = 2816
EXPERTS = 32
TOP_K = 2
TOK_MB = 256
DEVICES = 32
LAYERS = 2
MICRO_BATCHES = 2
CAPACITY = 2 * ((TOK_MB * TOP_K + EXPERTS - 1) // EXPERTS)
ROWS_MAX = DEVICES * CAPACITY
ROUTE_SCALE = 2.5


def rank_table():
    hot_count = EXPERTS // 16 + 1
    rest_total = TOK_MB * TOP_K - hot_count * CAPACITY
    cold_count = EXPERTS - hot_count
    base_share = rest_total // cold_count
    extra_count = rest_total % cold_count
    counts = [CAPACITY] * hot_count + [base_share + 1] * extra_count + [base_share] * (cold_count - extra_count)
    return np.repeat(np.arange(EXPERTS), counts).reshape(TOP_K, TOK_MB).T.astype(np.int32)


def route_block(key):
    key_perm, key_tok, key_roll = jax.random.split(key, 3)
    expert_perm = jax.random.permutation(key_perm, EXPERTS)
    chosen = expert_perm[jnp.asarray(rank_table())]
    chosen = chosen[jax.random.permutation(key_tok, TOK_MB)]
    roll_shift = jax.random.randint(key_roll, (TOK_MB, 1), 0, TOP_K)
    slot_order = (jnp.arange(TOP_K)[None, :] + roll_shift) % TOP_K
    return jnp.take_along_axis(chosen, slot_order, axis=1).astype(jnp.int32)


def setup_inputs(seed: int = 0) -> dict:
    key = jax.random.key(seed)
    key_x, key_ids, key_gate, key_up1, key_up3, key_down = jax.random.split(key, 6)
    n_tokens = DEVICES * TOK_MB
    tokens_in = jax.random.normal(key_x, (MICRO_BATCHES, n_tokens, HIDDEN), jnp.float32).astype(jnp.bfloat16)
    block_keys = jax.random.split(key_ids, LAYERS * MICRO_BATCHES * DEVICES)
    expert_ids = jax.vmap(route_block)(block_keys).reshape(LAYERS, MICRO_BATCHES, n_tokens, TOP_K)
    raw_gates = jax.random.uniform(key_gate, (LAYERS, MICRO_BATCHES, n_tokens, TOP_K), jnp.float32, 0.25, 1.75)
    gate_vals = raw_gates / jnp.sum(raw_gates, axis=-1, keepdims=True)
    up_shape = (LAYERS, EXPERTS, HIDDEN, FFN_DIM)
    w_up1 = (jax.random.normal(key_up1, up_shape, jnp.float32) * HIDDEN ** -0.5).astype(jnp.bfloat16)
    w_up3 = (jax.random.normal(key_up3, up_shape, jnp.float32) * HIDDEN ** -0.5).astype(jnp.bfloat16)
    w_down = (jax.random.normal(key_down, (LAYERS, EXPERTS, FFN_DIM, HIDDEN), jnp.float32) * FFN_DIM ** -0.5).astype(jnp.bfloat16)
    return {"tokens_in": tokens_in, "expert_ids": expert_ids, "gate_vals": gate_vals, "w_up1": w_up1, "w_up3": w_up3, "w_down": w_down}


def moe_layer(tokens, ids_mb, gates_mb, mat_up1, mat_up3, mat_down):
    n_assign = tokens.shape[0] * TOP_K
    flat_ids = ids_mb.reshape(n_assign)
    sort_order = jnp.argsort(flat_ids, stable=True)
    counts = jnp.bincount(flat_ids, length=EXPERTS)
    starts = jnp.cumsum(counts) - counts
    row_pos = jnp.arange(ROWS_MAX)

    def one_expert(operands):
        first_row, row_count, mat_a, mat_b, mat_c = operands
        picked = sort_order[jnp.minimum(first_row + row_pos, n_assign - 1)]
        expert_rows = tokens[picked // TOP_K]
        gate_in = jnp.dot(expert_rows, mat_a, preferred_element_type=jnp.float32)
        lin_in = jnp.dot(expert_rows, mat_b, preferred_element_type=jnp.float32)
        hidden = (jax.nn.silu(gate_in) * lin_in).astype(jnp.bfloat16)
        expert_out = jnp.dot(hidden, mat_c, preferred_element_type=jnp.float32).astype(jnp.bfloat16)
        return expert_out, jnp.where(row_pos < row_count, picked, n_assign)

    all_out, targets = lax.map(one_expert, (starts, counts, mat_up1, mat_up3, mat_down))
    per_assign = jnp.zeros((n_assign + 1, HIDDEN), jnp.bfloat16).at[targets.reshape(-1)].set(all_out.reshape(-1, HIDDEN))
    per_assign = per_assign[:n_assign].reshape(tokens.shape[0], TOP_K, HIDDEN)
    moe_sum = jnp.einsum("tj,tjh->th", gates_mb.astype(jnp.float32), per_assign.astype(jnp.float32))
    return (tokens.astype(jnp.float32) + ROUTE_SCALE * moe_sum).astype(jnp.bfloat16)


def reference(tokens_in, expert_ids, gate_vals, w_up1, w_up3, w_down):
    def layer_step(layer_in, layer_args):
        ids_layer, gates_layer, mat_up1, mat_up3, mat_down = layer_args

        def one_batch(batch_args):
            batch_tok, ids_mb, gates_mb = batch_args
            return moe_layer(batch_tok, ids_mb, gates_mb, mat_up1, mat_up3, mat_down)

        return lax.map(one_batch, (layer_in, ids_layer, gates_layer)), None

    tokens_out, _ = lax.scan(layer_step, tokens_in, (expert_ids, gate_vals, w_up1, w_up3, w_down))
    return tokens_out
```

```python
import functools

import jax
import jax.numpy as jnp
from jax import lax
from jax.experimental import pallas as pl
from jax.experimental.pallas import tpu as pltpu
from jax.sharding import PartitionSpec as P

ROUTE_SCALE = 2.5
MESH_AXES = ("ez", "ey", "ex")
NZ, NC = 4, 8
TILE = 256
BF16, F32 = jnp.bfloat16, jnp.float32
MESH = pl.DeviceIdType.MESH


def dot(lhs, rhs):
    return jnp.dot(lhs, rhs, preferred_element_type=F32)


def dot_t(lhs, rhs):
    return lax.dot_general(lhs, rhs, (((0,), (0,)), ((), ())), preferred_element_type=F32)


def moe_kernel(rows, tok_ref, grow_ref, prow_ref, gate_ref, w1_hbm, w3_hbm, wd_hbm, out_ref,
               ucur, tsend, trecv, ssend, xrecv, osend, rrecv, ysend, yrecv, w1, w3, wd, hid,
               w_sem, tz_s, tz_r, sp_s, sp_r, op_s, op_r, yz_s, yz_r):
    n_layers, n_mb = grow_ref.shape[0], grow_ref.shape[1]
    slots, width = NC * 32, ucur.shape[-1]
    ffn = w1.shape[-1]
    me_z = lax.axis_index("ez")
    me_c = lax.axis_index("ey") * 4 + lax.axis_index("ex")

    def peer_z(k):
        return 2 * ((me_z // 2 + k // 2) % 2) + (me_z % 2 + k % 2) % 2

    def peer_c(d):
        return (me_c + d) % NC

    def w_copies(layer):
        return [pltpu.make_async_copy(src.at[layer, 0], dst, w_sem.at[i])
                for i, (src, dst) in enumerate(((w1_hbm, w1), (w3_hbm, w3), (wd_hbm, wd)))]

    def t_copy(mb, k):
        return pltpu.make_async_remote_copy(
            src_ref=tsend.at[mb, k], dst_ref=trecv.at[mb, k], send_sem=tz_s.at[mb, k], recv_sem=tz_r.at[mb, k],
            device_id={"ez": peer_z(k)}, device_id_type=MESH)

    def y_copy(mb, k):
        return pltpu.make_async_remote_copy(
            src_ref=ysend.at[mb, k], dst_ref=yrecv.at[mb, me_z], send_sem=yz_s.at[mb, k], recv_sem=yz_r.at[mb, me_z],
            device_id={"ez": peer_z(k)}, device_id_type=MESH)

    def y_wait(mb, k):
        src = peer_z(k)
        pltpu.make_async_remote_copy(
            src_ref=ysend.at[mb, k], dst_ref=yrecv.at[mb, src], send_sem=yz_s.at[mb, k], recv_sem=yz_r.at[mb, src],
            device_id={"ez": src}, device_id_type=MESH).wait_recv()

    def plane_copy(src, dst, s_sem, r_sem, mb, k, d):
        c = peer_c(d)
        return pltpu.make_async_remote_copy(
            src_ref=src.at[mb, k, c], dst_ref=dst.at[mb, k, me_c], send_sem=s_sem.at[mb, k], recv_sem=r_sem.at[mb, k],
            device_id={"ey": c // 4, "ex": c % 4}, device_id_type=MESH)

    def plane_all(src, dst, s_sem, r_sem, mb, k):
        part = pl.ds(0, NC - 1)
        return pltpu.make_async_remote_copy(
            src_ref=src.at[mb, k, part], dst_ref=dst.at[mb, k, part], send_sem=s_sem.at[mb, k],
            recv_sem=r_sem.at[mb, k], device_id={"ey": peer_c(1) // 4, "ex": peer_c(1) % 4}, device_id_type=MESH)

    def one_hot(cond):
        return jnp.where(cond, 1.0, 0.0).astype(BF16)

    def send_tokens(layer, mb):
        g0 = grow_ref[layer, mb, 0:1, :]
        g1 = grow_ref[layer, mb, 1:2, :]
        tok = ucur[mb]
        for k in (1, 2, 3, 0):
            base = peer_z(k) * rows
            row = lax.broadcasted_iota(jnp.int32, (rows, tok.shape[0]), 0) + base
            packed = dot(one_hot((row == g0) | (row == g1)), tok).astype(BF16)
            if k == 0:
                trecv[mb, 0] = packed
            else:
                tsend[mb, k] = packed
                t_copy(mb, k).start()

    def expand_matrix(layer, mb, k):
        row = lax.broadcasted_iota(jnp.int32, (rows, slots), 0)
        return one_hot(row == prow_ref[layer, mb, k:k + 1, :])

    def expand(layer, mb, k):
        if k:
            t_copy(mb, k).wait_recv()
        ssend[mb, k] = dot_t(expand_matrix(layer, mb, k), trecv[mb, k]).astype(BF16).reshape(NC, 32, width)
        for d in range(1, NC):
            plane_copy(ssend, xrecv, sp_s, sp_r, mb, k, d).start()
        xrecv[mb, k, me_c] = ssend[mb, k, me_c]

    def expert(mb, k):
        plane_all(ssend, xrecv, sp_s, sp_r, mb, k).wait_recv()

        def up(t, _):
            cols = pl.ds(pl.multiple_of(t * TILE, TILE), TILE)
            x = xrecv[mb, k].reshape(slots, width)
            a = dot(x, w1[:, cols])
            b = dot(x, w3[:, cols])
            hid[:, cols] = (jax.nn.silu(a) * b).astype(BF16)
            return 0

        lax.fori_loop(0, ffn // TILE, up, 0)

        def down(t, _):
            cols = pl.ds(pl.multiple_of(t * TILE, TILE), TILE)
            osend[mb, k, :, :, cols] = dot(hid[...], wd[:, cols]).astype(BF16).reshape(NC, 32, TILE)
            return 0

        lax.fori_loop(0, width // TILE, down, 0)
        for d in range(1, NC):
            plane_copy(osend, rrecv, op_s, op_r, mb, k, d).start()
        rrecv[mb, k, me_c] = osend[mb, k, me_c]

    def give_back(layer, mb, k):
        plane_all(osend, rrecv, op_s, op_r, mb, k).wait_recv()
        packed = dot(expand_matrix(layer, mb, k), rrecv[mb, k].reshape(slots, width)).astype(BF16)
        if k == 0:
            yrecv[mb, me_z] = packed
        else:
            ysend[mb, k] = packed
            y_copy(mb, k).start()

    def combine(layer, mb):
        for k in (1, 2, 3):
            y_wait(mb, k)
        y = yrecv[mb].reshape(NZ * rows, width)
        row = lax.broadcasted_iota(jnp.int32, (NZ * rows, ucur.shape[1]), 0)
        total = jnp.zeros(ucur.shape[1:], F32)
        for j in range(2):
            picked = dot_t(one_hot(row == grow_ref[layer, mb, j:j + 1, :]), y)
            total = total + gate_ref[layer, :, 2 * mb + j:2 * mb + j + 1] * picked
        ucur[mb] = (ucur[mb].astype(F32) + ROUTE_SCALE * total).astype(BF16)
        for k in range(NZ):
            if k:
                t_copy(mb, k).wait_send()
                y_copy(mb, k).wait_send()
            plane_all(ssend, xrecv, sp_s, sp_r, mb, k).wait_send()
            plane_all(osend, rrecv, op_s, op_r, mb, k).wait_send()

    for copy in w_copies(0):
        copy.start()
    ucur[...] = tok_ref[...]
    barrier = pltpu.get_barrier_semaphore()
    for k in range(1, NZ):
        pl.semaphore_signal(barrier, inc=1, device_id={"ez": peer_z(k)}, device_id_type=MESH)
    for d in range(1, NC):
        c = peer_c(d)
        pl.semaphore_signal(barrier, inc=1, device_id={"ey": c // 4, "ex": c % 4}, device_id_type=MESH)
    pl.semaphore_wait(barrier, NZ - 1 + NC - 1)

    send_tokens(0, 0)
    send_tokens(0, 1)

    def layer_step(layer, _):
        expand(layer, 0, 0)
        expand(layer, 1, 0)
        for copy in w_copies(layer):
            copy.wait()
        expert(0, 0)
        expand(layer, 0, 1)
        expert(1, 0)
        give_back(layer, 0, 0)
        expert(0, 1)
        expand(layer, 0, 2)
        give_back(layer, 0, 1)
        expert(0, 2)
        expand(layer, 0, 3)
        give_back(layer, 0, 2)
        expert(0, 3)
        give_back(layer, 1, 0)
        expand(layer, 1, 1)
        give_back(layer, 0, 3)
        expert(1, 1)
        expand(layer, 1, 2)
        give_back(layer, 1, 1)
        expert(1, 2)
        expand(layer, 1, 3)
        give_back(layer, 1, 2)
        expert(1, 3)

        @pl.when(layer + 1 < n_layers)
        def _():
            for copy in w_copies(layer + 1):
                copy.start()

        give_back(layer, 1, 3)
        for mb in range(n_mb):
            combine(layer, mb)

            @pl.when(layer + 1 < n_layers)
            def _():
                send_tokens(layer + 1, mb)
        return 0

    lax.fori_loop(0, n_layers, layer_step, 0)
    out_ref[...] = ucur[...]


def run_moe(rows, collective_id, tokens, grow, prow, gates, w_up1, w_up3, w_down):
    n_mb, n_tok, width = tokens.shape
    ffn = w_up1.shape[-1]
    vmem = pl.BlockSpec(memory_space=pltpu.VMEM)
    hbm = pl.BlockSpec(memory_space=pl.ANY)
    packed = pltpu.VMEM((n_mb, NZ, rows, width), BF16)
    padded = pltpu.VMEM((n_mb, NZ, NC, 32, width), BF16)
    pair = pltpu.SemaphoreType.DMA((n_mb, NZ))
    return pl.pallas_call(
        functools.partial(moe_kernel, rows),
        out_shape=jax.ShapeDtypeStruct(tokens.shape, BF16),
        in_specs=[vmem] * 4 + [hbm] * 3,
        out_specs=vmem,
        scratch_shapes=[
            pltpu.VMEM((n_mb, n_tok, width), BF16),
            packed, packed, padded, padded, padded, padded, packed, packed,
            pltpu.VMEM((width, ffn), BF16), pltpu.VMEM((width, ffn), BF16), pltpu.VMEM((ffn, width), BF16),
            pltpu.VMEM((NC * 32, ffn), BF16),
            pltpu.SemaphoreType.DMA((3,)),
        ] + [pair] * 8,
        compiler_params=pltpu.CompilerParams(
            collective_id=collective_id, has_side_effects=True, vmem_limit_bytes=67_000_000),
        name=f"moe_rows_{rows}",
    )(tokens, grow, prow, gates, w_up1, w_up3, w_down)


def solution(mesh):
    tok_spec = P(None, MESH_AXES, None)
    route_spec = P(None, None, MESH_AXES, None)
    weight_spec = P(None, MESH_AXES, None, None)

    def device_body(tokens_in, expert_ids, gate_vals, w_up1, w_up3, w_down):
        n_layers, n_mb, n_tok, top_k = expert_ids.shape
        experts = NZ * NC
        me_z = lax.axis_index("ez")
        me_c = lax.axis_index("ey") * 4 + lax.axis_index("ex")
        chosen = (expert_ids[..., None] == jnp.arange(experts)).astype(F32)
        per_tok = jnp.sum(chosen, axis=3)
        before = (jnp.arange(n_tok)[:, None] > jnp.arange(n_tok)[None, :]).astype(BF16)
        rank_e = jnp.einsum("ts,lmse->lmte", before, per_tok.astype(BF16), preferred_element_type=F32)
        counts = jnp.sum(per_tok, axis=2).astype(jnp.int32)
        by_plane = counts.reshape(n_layers, n_mb, NZ, NC)
        off_e = (jnp.cumsum(by_plane, axis=-1) - by_plane).reshape(n_layers, n_mb, experts)
        in_plane = jnp.sum(chosen * (rank_e + off_e[:, :, None, :].astype(F32))[:, :, :, None, :], axis=-1)
        in_plane = in_plane.astype(jnp.int32)
        plane = expert_ids // NC

        all_counts = lax.all_gather(by_plane, MESH_AXES)
        fits = jnp.max(jnp.sum(all_counts, axis=-1)) <= 176
        all_counts = all_counts.reshape(NZ, NC, n_layers, n_mb, NZ, NC)
        mine = lax.dynamic_index_in_dim(all_counts, me_c, 1, keepdims=False)
        mine = lax.dynamic_index_in_dim(mine, me_z, 3, keepdims=False)
        order = [2 * ((me_z // 2 + k // 2) % 2) + (me_z % 2 + k % 2) % 2 for k in range(NZ)]
        mine = jnp.stack([lax.dynamic_index_in_dim(mine, zs, 0, keepdims=False) for zs in order], axis=2)
        start = jnp.cumsum(mine, axis=-1) - mine
        lane = jnp.arange(32)
        prow = jnp.where(lane < mine[..., None], start[..., None] + lane, -1).reshape(n_layers, n_mb, NZ, NC * 32)
        gates = gate_vals.transpose(0, 2, 1, 3).reshape(n_layers, n_tok, n_mb * top_k)

        def branch(rows, collective_id):
            def run():
                grow = (plane * rows + in_plane).transpose(0, 1, 3, 2)
                return run_moe(rows, collective_id, tokens_in, grow, prow, gates, w_up1, w_up3, w_down)
            return run

        return lax.cond(fits, branch(176, 1), branch(256, 2))

    return jax.shard_map(device_body, mesh=mesh, in_specs=(tok_spec, route_spec, route_spec, weight_spec, weight_spec, weight_spec), out_specs=tok_spec, check_vma=False)
```

```python
import functools

import jax
import jax.numpy as jnp
from jax import lax
from jax.experimental import pallas as pl
from jax.experimental.pallas import tpu as pltpu
from jax.sharding import PartitionSpec as P

ROUTE_SCALE = 2.5
MESH_AXES = ("ez", "ey", "ex")
NZ, NC, CAP = 4, 8, 32
EXPERTS, SLOTS = NZ * NC, NC * CAP
TILE = 256
BF16, F32 = jnp.bfloat16, jnp.float32
MESH = pl.DeviceIdType.MESH


def dot(lhs, rhs):
    return jnp.dot(lhs, rhs, preferred_element_type=F32)


def dot_t(lhs, rhs):
    return lax.dot_general(lhs, rhs, (((0,), (0,)), ((), ())), preferred_element_type=F32)


def dot_nt(lhs, rhs):
    return lax.dot_general(lhs, rhs, (((1,), (1,)), ((), ())), preferred_element_type=F32)


def one_hot(cond):
    return jnp.where(cond, 1.0, 0.0).astype(BF16)


def iota(shape, dim):
    return lax.broadcasted_iota(jnp.int32, shape, dim)


def place():
    return lax.axis_index("ez"), lax.axis_index("ey") * 4 + lax.axis_index("ex")


def peer_of(me_z, k):
    return 2 * ((me_z // 2 + k // 2) % 2) + (me_z % 2 + k % 2) % 2


def plane_id(c):
    return {"ey": c // 4, "ex": c % 4}


def route_kernel(ids_ref, meta_ref, prow_ref, peak_ref, mine, seen, s_sem, r_sem):
    n_layers, n_mb, n_tok, top_k = ids_ref.shape
    lanes = n_layers * n_mb * EXPERTS
    me_z, me_c = place()
    me = me_z * NC + me_c
    n_dev = NZ * NC

    def target(d):
        dev = (me + d) % n_dev
        return {"ez": dev // NC, "ey": dev % NC // 4, "ex": dev % 4}

    barrier = pltpu.get_barrier_semaphore()

    def greet(d, _):
        pl.semaphore_signal(barrier, inc=1, device_id=target(d), device_id_type=MESH)
        return 0

    lax.fori_loop(1, n_dev, greet, 0)

    lane = iota((n_tok, lanes), 1)
    chosen = []
    for j in range(top_k):
        ids = jnp.zeros((n_tok, lanes), jnp.int32)
        for layer in range(n_layers):
            for mb in range(n_mb):
                ids = jnp.where(lane // EXPERTS == layer * n_mb + mb, ids_ref[layer, mb, :, j:j + 1], ids)
        chosen.append(jnp.where(ids == lane % EXPERTS, 1.0, 0.0))
    per_tok = (chosen[0] + chosen[1]).astype(BF16)
    counts = dot(jnp.ones((8, n_tok), BF16), per_tok)
    mine[...] = counts
    seen[me] = counts
    pl.semaphore_wait(barrier, n_dev - 1)

    def share(d, _):
        pltpu.make_async_remote_copy(src_ref=mine, dst_ref=seen.at[me], send_sem=s_sem, recv_sem=r_sem,
                                     device_id=target(d), device_id_type=MESH).start()
        return 0

    lax.fori_loop(1, n_dev, share, 0)

    before = one_hot(iota((n_tok, n_tok), 0) > iota((n_tok, n_tok), 1))
    rank = dot(before, per_tok)
    row, col = iota((lanes, lanes), 0), iota((lanes, lanes), 1)
    same_plane = row // NC == col // NC
    start = dot(counts.astype(BF16), one_hot(same_plane & (row < col)))[0:1]
    pick = one_hot(iota((8, lanes), 0) == iota((8, lanes), 1) // EXPERTS)
    for j in range(top_k):
        base = dot_nt(pick, (chosen[j] * (lane % EXPERTS // NC).astype(F32)).astype(BF16)) * SLOTS
        packed = base + dot_nt(pick, (chosen[j] * (rank + start)).astype(BF16))
        padded = base + dot_nt(pick, (chosen[j] * (rank + (lane % NC * CAP).astype(F32))).astype(BF16))
        for layer in range(n_layers):
            for mb in range(n_mb):
                i = layer * n_mb + mb
                meta_ref[layer, mb, j:j + 1, :] = packed[i:i + 1].astype(jnp.int32)
                meta_ref[layer, mb, top_k + j:top_k + j + 1, :] = padded[i:i + 1].astype(jnp.int32)

    rest = pltpu.make_async_remote_copy(
        src_ref=seen.at[pl.ds(0, n_dev - 1)], dst_ref=seen.at[pl.ds(0, n_dev - 1)], send_sem=s_sem, recv_sem=r_sem,
        device_id=target(1), device_id_type=MESH)
    rest.wait_recv()
    everyone = seen[...].reshape(n_dev * 8, lanes).astype(BF16)
    loads = dot(everyone, one_hot(same_plane))
    peak_ref[...] = jnp.broadcast_to(jnp.max(loads, axis=0, keepdims=True), peak_ref.shape)
    sources = jnp.concatenate([seen[peer_of(me_z, k) * NC + me_c] for k in range(NZ)], axis=0).astype(BF16)
    lane_of, slot_of = iota((lanes, SLOTS), 0), iota((lanes, SLOTS), 1)
    within = iota((NZ * 8, SLOTS), 1) % CAP
    for layer in range(n_layers):
        for mb in range(n_mb):
            first = (layer * n_mb + mb) * EXPERTS + me_z * NC
            own = lane_of - first
            amount = dot(sources, one_hot(own == slot_of // CAP)).astype(jnp.int32)
            ahead = dot(sources, one_hot((own >= 0) & (own < slot_of // CAP))).astype(jnp.int32)
            prow_ref[layer, mb] = jnp.where(within < amount, ahead + within, -1).reshape(NZ, 8, SLOTS)
    rest.wait_send()


def moe_kernel(rows, tok_ref, meta_ref, prow_ref, gate_ref, w1_hbm, w3_hbm, wd_hbm, out_ref,
               ucur, pmeta, tsend, trecv, tfull, ssend, xrecv, osend, rrecv, ysend, yrecv, w1, w3, wd, hid,
               w_sem, m_sem, tz_s, tz_r, tf_s, tf_r, sp_s, sp_r, op_s, op_r, yz_s, yz_r):
    n_layers, n_mb = meta_ref.shape[0], meta_ref.shape[1]
    n_tok, width = ucur.shape[1:]
    ffn = w1.shape[-1]
    me_z, me_c = place()
    peer_z = functools.partial(peer_of, me_z)

    def peer_c(d):
        return (me_c + d) % NC

    def w_copies(layer):
        return [pltpu.make_async_copy(src.at[layer, 0], dst, w_sem.at[i])
                for i, (src, dst) in enumerate(((w1_hbm, w1), (w3_hbm, w3), (wd_hbm, wd)))]

    meta_copy = pltpu.make_async_remote_copy(
        src_ref=meta_ref, dst_ref=pmeta, send_sem=m_sem.at[0], recv_sem=m_sem.at[1],
        device_id={"ez": peer_z(2)}, device_id_type=MESH)

    def t_copy(mb, i):
        return pltpu.make_async_remote_copy(
            src_ref=tsend.at[mb, i], dst_ref=trecv.at[mb, i], send_sem=tz_s.at[mb, i], recv_sem=tz_r.at[mb, i],
            device_id={"ez": peer_z(1)}, device_id_type=MESH)

    def full_copy(mb):
        return pltpu.make_async_remote_copy(
            src_ref=ucur.at[mb], dst_ref=tfull.at[mb], send_sem=tf_s.at[mb], recv_sem=tf_r.at[mb],
            device_id={"ez": peer_z(2)}, device_id_type=MESH)

    def y_copy(mb, k):
        return pltpu.make_async_remote_copy(
            src_ref=ysend.at[mb, k], dst_ref=yrecv.at[mb, me_z], send_sem=yz_s.at[mb, k], recv_sem=yz_r.at[mb, me_z],
            device_id={"ez": peer_z(k)}, device_id_type=MESH)

    def y_wait(mb, k):
        src = peer_z(k)
        pltpu.make_async_remote_copy(
            src_ref=ysend.at[mb, k], dst_ref=yrecv.at[mb, src], send_sem=yz_s.at[mb, k], recv_sem=yz_r.at[mb, src],
            device_id={"ez": src}, device_id_type=MESH).wait_recv()

    def plane_copy(src, dst, s_sem, r_sem, mb, k, d):
        c = peer_c(d)
        return pltpu.make_async_remote_copy(
            src_ref=src.at[mb, k, c], dst_ref=dst.at[mb, k, me_c], send_sem=s_sem.at[mb, k], recv_sem=r_sem.at[mb, k],
            device_id=plane_id(c), device_id_type=MESH)

    def plane_all(src, dst, s_sem, r_sem, mb, k):
        part = pl.ds(0, NC - 1)
        return pltpu.make_async_remote_copy(
            src_ref=src.at[mb, k, part], dst_ref=dst.at[mb, k, part], send_sem=s_sem.at[mb, k],
            recv_sem=r_sem.at[mb, k], device_id=plane_id(peer_c(1)), device_id_type=MESH)

    def choose(ref, layer, mb, j, n, base):
        row = iota((n, n_tok), 0) + base
        return one_hot((row == ref[layer, mb, j:j + 1, :]) | (row == ref[layer, mb, j + 1:j + 2, :]))

    def send_tokens(layer, mb):
        full_copy(mb).start()
        tsend[mb, 0] = dot(choose(meta_ref, layer, mb, 0, rows, peer_z(1) * SLOTS), ucur[mb]).astype(BF16)
        t_copy(mb, 0).start()

    def packing(layer, mb, k):
        return one_hot(iota((rows, SLOTS), 0) == prow_ref[layer, mb, k, 0:1, :])

    def expand(layer, mb, k):
        if k == 0:
            block = dot(choose(meta_ref, layer, mb, 2, SLOTS, me_z * SLOTS), ucur[mb])
        elif k == 2:
            full_copy(mb).wait_recv()
            tsend[mb, 1] = dot(choose(pmeta, layer, mb, 0, rows, peer_z(1) * SLOTS), tfull[mb]).astype(BF16)
            t_copy(mb, 1).start()
            block = dot(choose(pmeta, layer, mb, 2, SLOTS, me_z * SLOTS), tfull[mb])
        else:
            t_copy(mb, k // 2).wait_recv()
            block = dot_t(packing(layer, mb, k), trecv[mb, k // 2])
        ssend[mb, k] = block.astype(BF16).reshape(NC, CAP, width)
        for d in range(1, NC):
            plane_copy(ssend, xrecv, sp_s, sp_r, mb, k, d).start()
        xrecv[mb, k, me_c] = ssend[mb, k, me_c]

    def expert(mb, k):
        plane_all(ssend, xrecv, sp_s, sp_r, mb, k).wait_recv()

        def up(t, _):
            cols = pl.ds(pl.multiple_of(t * TILE, TILE), TILE)
            x = xrecv[mb, k].reshape(SLOTS, width)
            a = dot(x, w1[:, cols])
            b = dot(x, w3[:, cols])
            hid[:, cols] = (jax.nn.silu(a) * b).astype(BF16)
            return 0

        lax.fori_loop(0, ffn // TILE, up, 0, unroll=True)

        def down(t, _):
            cols = pl.ds(pl.multiple_of(t * TILE, TILE), TILE)
            osend[mb, k, :, :, cols] = dot(hid[...], wd[:, cols]).astype(BF16).reshape(NC, CAP, TILE)
            return 0

        lax.fori_loop(0, width // TILE, down, 0, unroll=True)
        for d in range(1, NC):
            plane_copy(osend, rrecv, op_s, op_r, mb, k, d).start()
        rrecv[mb, k, me_c] = osend[mb, k, me_c]

    def give_back(layer, mb, k):
        plane_all(osend, rrecv, op_s, op_r, mb, k).wait_recv()
        packed = dot(packing(layer, mb, k), rrecv[mb, k].reshape(SLOTS, width)).astype(BF16)

        @pl.when(k == 0)
        def _():
            yrecv[mb, me_z] = packed

        @pl.when(k > 0)
        def _():
            ysend[mb, k] = packed
            y_copy(mb, k).start()

    def combine(layer, mb):
        full_copy(mb).wait_send()
        for k in (1, 2, 3):
            y_wait(mb, k)
        y = yrecv[mb].reshape(NZ * rows, width)
        shape = (NZ, rows, n_tok)
        row = (iota(shape, 0) * SLOTS + iota(shape, 1)).reshape(NZ * rows, n_tok)
        total = jnp.zeros((n_tok, width), F32)
        for j in range(2):
            picked = dot_t(one_hot(row == meta_ref[layer, mb, j:j + 1, :]), y)
            total = total + gate_ref[layer, mb, :, j:j + 1] * picked
        ucur[mb] = (ucur[mb].astype(F32) + ROUTE_SCALE * total).astype(BF16)
        for i in range(2):
            t_copy(mb, i).wait_send()
        for k in range(NZ):
            if k:
                y_copy(mb, k).wait_send()
            plane_all(ssend, xrecv, sp_s, sp_r, mb, k).wait_send()
            plane_all(osend, rrecv, op_s, op_r, mb, k).wait_send()

    barrier = pltpu.get_barrier_semaphore()
    for k in range(1, NZ):
        pl.semaphore_signal(barrier, inc=1, device_id={"ez": peer_z(k)}, device_id_type=MESH)
    for d in range(1, NC):
        pl.semaphore_signal(barrier, inc=1, device_id=plane_id(peer_c(d)), device_id_type=MESH)
    for copy in w_copies(0):
        copy.start()
    ucur[...] = tok_ref[...]
    pl.semaphore_wait(barrier, NZ - 1 + NC - 1)
    meta_copy.start()
    for mb in range(n_mb):
        send_tokens(0, mb)
    meta_copy.wait_recv()
    n_step = n_mb * NZ

    def layer_step(layer, _):
        expand(layer, 0, 0)

        def step(j, _):
            for k in range(NZ):
                @pl.when((j + 1 < n_step) & ((j + 1) % NZ == k))
                def _():
                    expand(layer, (j + 1) // NZ, k)

            @pl.when(j == 0)
            def _():
                for copy in w_copies(layer):
                    copy.wait()

            expert(j // NZ, j % NZ)

            @pl.when((j == n_step - 1) & (layer + 1 < n_layers))
            def _():
                for copy in w_copies(layer + 1):
                    copy.start()

            @pl.when(j > 0)
            def _():
                give_back(layer, (j - 1) // NZ, (j - 1) % NZ)
            return 0

        lax.fori_loop(0, n_step, step, 0)
        give_back(layer, n_mb - 1, NZ - 1)

        for mb in range(n_mb):
            combine(layer, mb)

            @pl.when(layer + 1 < n_layers)
            def _():
                send_tokens(layer + 1, mb)
        return 0

    lax.fori_loop(0, n_layers, layer_step, 0)
    meta_copy.wait_send()
    out_ref[...] = ucur[...]


VMEM_SPEC = pl.BlockSpec(memory_space=pltpu.VMEM)


def run_route(ids):
    n_layers, n_mb, n_tok, top_k = ids.shape
    lanes = n_layers * n_mb * EXPERTS
    return pl.pallas_call(
        route_kernel,
        out_shape=(jax.ShapeDtypeStruct((n_layers, n_mb, 2 * top_k, n_tok), jnp.int32),
                   jax.ShapeDtypeStruct((n_layers, n_mb, NZ, 8, SLOTS), jnp.int32),
                   jax.ShapeDtypeStruct((8, lanes), F32)),
        in_specs=[VMEM_SPEC],
        out_specs=(VMEM_SPEC,) * 3,
        scratch_shapes=[pltpu.VMEM((8, lanes), F32), pltpu.VMEM((NZ * NC, 8, lanes), F32),
                        pltpu.SemaphoreType.DMA, pltpu.SemaphoreType.DMA],
        compiler_params=pltpu.CompilerParams(collective_id=0, has_side_effects=True),
        name="route",
    )(ids)


def run_moe(rows, collective_id, tokens, meta, prow, gates, w_up1, w_up3, w_down):
    n_mb, n_tok, width = tokens.shape
    ffn = w_up1.shape[-1]
    hbm = pl.BlockSpec(memory_space=pl.ANY)
    per_mb = pltpu.VMEM((n_mb, n_tok, width), BF16)
    relay = pltpu.VMEM((n_mb, 2, rows, width), BF16)
    packed = pltpu.VMEM((n_mb, NZ, rows, width), BF16)
    padded = pltpu.VMEM((n_mb, NZ, NC, CAP, width), BF16)
    pair = pltpu.SemaphoreType.DMA((n_mb, NZ))
    return pl.pallas_call(
        functools.partial(moe_kernel, rows),
        out_shape=jax.ShapeDtypeStruct(tokens.shape, BF16),
        in_specs=[VMEM_SPEC] * 4 + [hbm] * 3,
        out_specs=VMEM_SPEC,
        scratch_shapes=[
            per_mb, pltpu.VMEM(meta.shape, jnp.int32), relay, relay, per_mb,
            padded, padded, padded, padded, packed, packed,
            pltpu.VMEM((width, ffn), BF16), pltpu.VMEM((width, ffn), BF16), pltpu.VMEM((ffn, width), BF16),
            pltpu.VMEM((SLOTS, ffn), BF16),
            pltpu.SemaphoreType.DMA((3,)), pltpu.SemaphoreType.DMA((2,)),
            pltpu.SemaphoreType.DMA((n_mb, 2)), pltpu.SemaphoreType.DMA((n_mb, 2)),
            pltpu.SemaphoreType.DMA((n_mb,)), pltpu.SemaphoreType.DMA((n_mb,)),
        ] + [pair] * 6,
        compiler_params=pltpu.CompilerParams(
            collective_id=collective_id, has_side_effects=True, vmem_limit_bytes=67_000_000),
        name=f"moe_rows_{rows}",
    )(tokens, meta, prow, gates, w_up1, w_up3, w_down)


def solution(mesh):
    tok_spec = P(None, MESH_AXES, None)
    route_spec = P(None, None, MESH_AXES, None)
    weight_spec = P(None, MESH_AXES, None, None)

    def device_body(tokens_in, expert_ids, gate_vals, w_up1, w_up3, w_down):
        meta, prow, peak = run_route(expert_ids)

        def branch(rows, collective_id):
            return lambda: run_moe(rows, collective_id, tokens_in, meta, prow, gate_vals, w_up1, w_up3, w_down)

        return lax.cond(jnp.max(peak) <= 176.0, branch(176, 1), branch(SLOTS, 2))

    return jax.shard_map(device_body, mesh=mesh, in_specs=(tok_spec, route_spec, route_spec, weight_spec, weight_spec, weight_spec), out_specs=tok_spec, check_vma=False)
```

```python
import functools

import jax
import jax.numpy as jnp
from jax import lax
from jax.experimental import pallas as pl
from jax.experimental.pallas import tpu as pltpu
from jax.sharding import PartitionSpec as P

ROUTE_SCALE = 2.5
MESH_AXES = ("ez", "ey", "ex")
NZ, NC, CAP = 4, 8, 32
EXPERTS, SLOTS = NZ * NC, NC * CAP
TILE = 256
BF16, F32 = jnp.bfloat16, jnp.float32
MESH = pl.DeviceIdType.MESH


def dot(lhs, rhs):
    return jnp.dot(lhs, rhs, preferred_element_type=F32)


def dot_t(lhs, rhs):
    return lax.dot_general(lhs, rhs, (((0,), (0,)), ((), ())), preferred_element_type=F32)


def dot_nt(lhs, rhs):
    return lax.dot_general(lhs, rhs, (((1,), (1,)), ((), ())), preferred_element_type=F32)


def one_hot(cond):
    return jnp.where(cond, 1.0, 0.0).astype(BF16)


def iota(shape, dim):
    return lax.broadcasted_iota(jnp.int32, shape, dim)


def place():
    return lax.axis_index("ez"), lax.axis_index("ey") * 4 + lax.axis_index("ex")


def source_of(me_z, k):
    half, far = me_z // 2, k // 2
    near = (1 - k) * me_z + k * (4 * half + 1 - me_z)
    away = (3 - k) * (2 - half) + (k - 2) * (3 - 3 * half)
    return (1 - far) * near + far * away


def plane_id(c):
    return {"ey": c // 4, "ex": c % 4}


def route_kernel(ids_ref, meta_ref, prow_ref, peak_ref, mine, seen, s_sem, r_sem):
    n_layers, n_mb, top_k, n_tok = ids_ref.shape
    n_set = n_layers * n_mb
    lanes = n_set * EXPERTS
    me_z, me_c = place()
    me = me_z * NC + me_c
    n_dev = NZ * NC

    def target(d):
        dev = (me + d) % n_dev
        return {"ez": dev // NC, "ey": dev % NC // 4, "ex": dev % 4}

    barrier = pltpu.get_barrier_semaphore()

    def greet(d, _):
        pl.semaphore_signal(barrier, inc=1, device_id=target(d), device_id_type=MESH)
        return 0

    lax.fori_loop(1, n_dev, greet, 0)

    expert = iota((EXPERTS, n_tok), 0)
    chosen = [jnp.concatenate([jnp.where(ids_ref[i // n_mb, i % n_mb, j:j + 1, :] == expert, 1.0, 0.0)
                               for i in range(n_set)], axis=0) for j in range(top_k)]
    per_tok = (chosen[0] + chosen[1]).astype(BF16)
    counts = dot_nt(jnp.ones((8, n_tok), BF16), per_tok)
    mine[...] = counts
    seen[me] = counts
    pl.semaphore_wait(barrier, n_dev - 1)

    def share(d, _):
        pltpu.make_async_remote_copy(src_ref=mine, dst_ref=seen.at[me], send_sem=s_sem, recv_sem=r_sem,
                                     device_id=target(d), device_id_type=MESH).start()
        return 0

    lax.fori_loop(1, n_dev, share, 0)

    rank = dot(per_tok, one_hot(iota((n_tok, n_tok), 0) < iota((n_tok, n_tok), 1)))
    totals = dot(per_tok, jnp.ones((n_tok, n_tok), BF16)).astype(BF16)
    row, col = iota((lanes, lanes), 0), iota((lanes, lanes), 1)
    same_plane = row // NC == col // NC
    start = dot(one_hot(same_plane & (col < row)), totals)
    which = iota((lanes, n_tok), 0) % EXPERTS
    base = which // NC * SLOTS
    packed = base.astype(F32) + rank + start
    padded = (base + which % NC * CAP).astype(F32) + rank
    for j in range(top_k):
        for i in range(n_set):
            part = slice(i * EXPERTS, (i + 1) * EXPERTS)
            for place_of, at in ((packed, j), (padded, top_k + j)):
                found = jnp.sum(chosen[j][part] * place_of[part], axis=0, keepdims=True)
                meta_ref[i // n_mb, i % n_mb, at:at + 1, :] = found.astype(jnp.int32)

    rest = pltpu.make_async_remote_copy(
        src_ref=seen.at[pl.ds(0, n_dev - 1)], dst_ref=seen.at[pl.ds(0, n_dev - 1)], send_sem=s_sem, recv_sem=r_sem,
        device_id=target(1), device_id_type=MESH)
    rest.wait_recv()
    everyone = seen[...].reshape(n_dev * 8, lanes).astype(BF16)
    loads = dot(everyone, one_hot(same_plane))
    peak_ref[0] = jnp.max(loads)
    sources = jnp.concatenate([seen[source_of(me_z, k) * NC + me_c] for k in range(NZ)], axis=0).astype(BF16)
    lane_of, slot_of = iota((lanes, SLOTS), 0), iota((lanes, SLOTS), 1)
    within = iota((NZ * 8, SLOTS), 1) % CAP
    for i in range(n_set):
        own = lane_of - (i * EXPERTS + me_z * NC)
        amount = dot(sources, one_hot(own == slot_of // CAP)).astype(jnp.int32)
        ahead = dot(sources, one_hot((own >= 0) & (own < slot_of // CAP))).astype(jnp.int32)
        prow_ref[i // n_mb, i % n_mb] = jnp.where(within < amount, ahead + within, -1).reshape(NZ, 8, SLOTS)
    rest.wait_send()


def moe_kernel(rows, tok_ref, meta_ref, prow_ref, gate_ref, w1_hbm, w3_hbm, wd_hbm, out_ref,
               ucur, gcol, pmeta, tsend, trecv, tfull, ssend, xrecv, osend, rrecv, ysend, yrecv, w1, w3, wd, hid,
               w_sem, m_s, m_r, tz_s, tz_r, tf_s, tf_r, sp_s, sp_r, op_s, op_r, yz_s, yz_r):
    n_layers, n_mb = meta_ref.shape[0], meta_ref.shape[1]
    n_tok, width = ucur.shape[1:]
    ffn = w1.shape[-1]
    me_z, me_c = place()
    source = functools.partial(source_of, me_z)
    near = source(1)
    gateway = source(2)
    inner = (me_z + 1) // 2 % 2
    my_far = 1 - inner

    def peer_c(d):
        return (me_c + d) % NC

    def w_copies(layer):
        return [pltpu.make_async_copy(src.at[layer, 0], dst, w_sem.at[i])
                for i, (src, dst) in enumerate(((w1_hbm, w1), (w3_hbm, w3), (wd_hbm, wd)))]

    def meta_copy(i):
        return pltpu.make_async_remote_copy(
            src_ref=meta_ref, dst_ref=pmeta.at[i], send_sem=m_s.at[0], recv_sem=m_r.at[i],
            device_id={"ez": gateway}, device_id_type=MESH)

    def t_copy(mb, i):
        return pltpu.make_async_remote_copy(
            src_ref=tsend.at[mb, i], dst_ref=trecv.at[mb, i], send_sem=tz_s.at[mb, i], recv_sem=tz_r.at[mb, i],
            device_id={"ez": near}, device_id_type=MESH)

    def full_copy(mb, i):
        return pltpu.make_async_remote_copy(
            src_ref=ucur.at[mb], dst_ref=tfull.at[mb, i], send_sem=tf_s.at[mb], recv_sem=tf_r.at[mb, i],
            device_id={"ez": gateway}, device_id_type=MESH)

    def y_copy(mb, k):
        return pltpu.make_async_remote_copy(
            src_ref=ysend.at[mb, k], dst_ref=yrecv.at[mb, me_z], send_sem=yz_s.at[mb, k], recv_sem=yz_r.at[mb, me_z],
            device_id={"ez": source(k)}, device_id_type=MESH)

    def y_wait(mb, k):
        src = source(k)
        pltpu.make_async_remote_copy(
            src_ref=ysend.at[mb, k], dst_ref=yrecv.at[mb, src], send_sem=yz_s.at[mb, k], recv_sem=yz_r.at[mb, src],
            device_id={"ez": src}, device_id_type=MESH).wait_recv()

    def plane_copy(src, dst, s_sem, r_sem, mb, k, d):
        c = peer_c(d)
        return pltpu.make_async_remote_copy(
            src_ref=src.at[mb, k, c], dst_ref=dst.at[mb, k, me_c], send_sem=s_sem.at[mb, k], recv_sem=r_sem.at[mb, k],
            device_id=plane_id(c), device_id_type=MESH)

    def plane_all(src, dst, s_sem, r_sem, mb, k):
        part = pl.ds(0, NC - 1)
        return pltpu.make_async_remote_copy(
            src_ref=src.at[mb, k, part], dst_ref=dst.at[mb, k, part], send_sem=s_sem.at[mb, k],
            recv_sem=r_sem.at[mb, k], device_id=plane_id(peer_c(1)), device_id_type=MESH)

    def choose(ref, j, n, base):
        row = iota((n, n_tok), 0) + base
        return one_hot((row == ref[j:j + 1, :]) | (row == ref[j + 1:j + 2, :]))

    def send_tokens(layer, mb):
        tsend[mb, 0] = dot(choose(meta_ref.at[layer, mb], 0, rows, near * SLOTS), ucur[mb]).astype(BF16)
        t_copy(mb, 0).start()
        full_copy(mb, my_far).start()

    def packing(layer, mb, k):
        return one_hot(iota((rows, SLOTS), 0) == prow_ref[layer, mb, k, 0:1, :])

    def spread(mb, k, block):
        ssend[mb, k] = block.astype(BF16).reshape(NC, CAP, width)
        for d in range(1, NC):
            plane_copy(ssend, xrecv, sp_s, sp_r, mb, k, d).start()
        xrecv[mb, k, me_c] = ssend[mb, k, me_c]

    def expand_own(layer, mb):
        spread(mb, 0, dot(choose(meta_ref.at[layer, mb], 2, SLOTS, me_z * SLOTS), ucur[mb]))

    def expand(layer, mb, k):
        def from_packed():
            t_copy(mb, k - 1).wait_recv()
            spread(mb, k, dot_t(packing(layer, mb, k), trecv[mb, k - 1]))

        @pl.when((k == 1) | (inner == 0))
        def _():
            from_packed()

        @pl.when((k > 1) & (inner == 1))
        def _():
            i = k - 2
            full_copy(mb, i).wait_recv()
            tsend[mb, k - 1] = dot(choose(pmeta.at[i, layer, mb], 0, rows, near * SLOTS), tfull[mb, i]).astype(BF16)
            t_copy(mb, k - 1).start()
            spread(mb, k, dot(choose(pmeta.at[i, layer, mb], 2, SLOTS, me_z * SLOTS), tfull[mb, i]))

    def expert(mb, k):
        plane_all(ssend, xrecv, sp_s, sp_r, mb, k).wait_recv()

        def up(t, _):
            cols = pl.ds(pl.multiple_of(t * TILE, TILE), TILE)
            x = xrecv[mb, k].reshape(SLOTS, width)
            a = dot(x, w1[:, cols])
            b = dot(x, w3[:, cols])
            hid[:, cols] = (jax.nn.silu(a) * b).astype(BF16)
            return 0

        lax.fori_loop(0, ffn // TILE, up, 0, unroll=True)

        def down(t, _):
            cols = pl.ds(pl.multiple_of(t * TILE, TILE), TILE)
            osend[mb, k, :, :, cols] = dot(hid[...], wd[:, cols]).astype(BF16).reshape(NC, CAP, TILE)
            return 0

        lax.fori_loop(0, width // TILE, down, 0, unroll=True)
        for d in range(1, NC):
            plane_copy(osend, rrecv, op_s, op_r, mb, k, d).start()
        rrecv[mb, k, me_c] = osend[mb, k, me_c]

    def give_back(layer, mb, k):
        plane_all(osend, rrecv, op_s, op_r, mb, k).wait_recv()
        packed = dot(packing(layer, mb, k), rrecv[mb, k].reshape(SLOTS, width)).astype(BF16)

        @pl.when(k == 0)
        def _():
            yrecv[mb, me_z] = packed

        @pl.when(k > 0)
        def _():
            ysend[mb, k] = packed
            y_copy(mb, k).start()

    def combine(layer, mb):
        full_copy(mb, my_far).wait_send()
        for k in (1, 2, 3):
            y_wait(mb, k)
        y = yrecv[mb].reshape(NZ * rows, width)
        shape = (NZ, rows, n_tok)
        row = (iota(shape, 0) * SLOTS + iota(shape, 1)).reshape(NZ * rows, n_tok)
        total = jnp.zeros((n_tok, width), F32)
        for j in range(2):
            picked = dot_t(one_hot(row == meta_ref[layer, mb, j:j + 1, :]), y)
            total = total + gcol[layer, :, 2 * mb + j:2 * mb + j + 1] * picked
        ucur[mb] = (ucur[mb].astype(F32) + ROUTE_SCALE * total).astype(BF16)
        t_copy(mb, 0).wait_send()

        @pl.when(inner == 1)
        def _():
            for i in (1, 2):
                t_copy(mb, i).wait_send()

        for k in range(NZ):
            if k:
                y_copy(mb, k).wait_send()
            plane_all(ssend, xrecv, sp_s, sp_r, mb, k).wait_send()
            plane_all(osend, rrecv, op_s, op_r, mb, k).wait_send()

    barrier = pltpu.get_barrier_semaphore()
    for k in range(1, NZ):
        pl.semaphore_signal(barrier, inc=1, device_id={"ez": source(k)}, device_id_type=MESH)
    for d in range(1, NC):
        pl.semaphore_signal(barrier, inc=1, device_id=plane_id(peer_c(d)), device_id_type=MESH)
    for copy in w_copies(0):
        copy.start()
    ucur[...] = tok_ref[...]
    n_gate = 2 * n_mb
    turned = jnp.transpose(gate_ref[...].reshape(n_layers * n_gate, n_tok))
    for layer in range(n_layers):
        gcol[layer] = turned[:, layer * n_gate:(layer + 1) * n_gate]
    pl.semaphore_wait(barrier, NZ - 1 + NC - 1)
    meta_copy(my_far).start()
    for mb in range(n_mb):
        send_tokens(0, mb)

    @pl.when(inner == 1)
    def _():
        for i in range(2):
            meta_copy(i).wait_recv()

    n_step = n_mb * NZ

    def chunk(j):
        later = (j + 6) // 8
        return later * ((j + 1) // 3 - 1) + (1 - later) * j, later * (1 + (j + 1) % 3)

    def layer_step(layer, _):
        for mb in range(n_mb):
            expand_own(layer, mb)
        for copy in w_copies(layer):
            copy.wait()

        def step(j, _):
            expert(*chunk(j))

            @pl.when((j == n_step - 1) & (layer + 1 < n_layers))
            def _():
                for copy in w_copies(layer + 1):
                    copy.start()

            @pl.when(j > 0)
            def _():
                give_back(layer, *chunk(j - 1))

            @pl.when(j + 2 < n_step)
            def _():
                expand(layer, *chunk(j + 2))
            return 0

        lax.fori_loop(0, n_step, step, 0)
        give_back(layer, n_mb - 1, NZ - 1)

        for mb in range(n_mb):
            combine(layer, mb)

            @pl.when(layer + 1 < n_layers)
            def _():
                send_tokens(layer + 1, mb)
        return 0

    lax.fori_loop(0, n_layers, layer_step, 0)
    meta_copy(my_far).wait_send()
    out_ref[...] = ucur[...]


VMEM_SPEC = pl.BlockSpec(memory_space=pltpu.VMEM)


def run_route(ids):
    n_layers, n_mb, top_k, n_tok = ids.shape
    lanes = n_layers * n_mb * EXPERTS
    return pl.pallas_call(
        route_kernel,
        out_shape=(jax.ShapeDtypeStruct((n_layers, n_mb, 2 * top_k, n_tok), jnp.int32),
                   jax.ShapeDtypeStruct((n_layers, n_mb, NZ, 8, SLOTS), jnp.int32),
                   jax.ShapeDtypeStruct((1,), F32)),
        in_specs=[VMEM_SPEC],
        out_specs=(VMEM_SPEC, VMEM_SPEC, pl.BlockSpec(memory_space=pltpu.SMEM)),
        scratch_shapes=[pltpu.VMEM((8, lanes), F32), pltpu.VMEM((NZ * NC, 8, lanes), F32),
                        pltpu.SemaphoreType.DMA, pltpu.SemaphoreType.DMA],
        compiler_params=pltpu.CompilerParams(collective_id=0, has_side_effects=True),
        name="route",
    )(ids)


def run_moe(rows, collective_id, tokens, meta, prow, gates, w_up1, w_up3, w_down):
    n_mb, n_tok, width = tokens.shape
    ffn = w_up1.shape[-1]
    hbm = pl.BlockSpec(memory_space=pl.ANY)
    per_mb = pltpu.VMEM((n_mb, n_tok, width), BF16)
    relay = pltpu.VMEM((n_mb, 3, rows, width), BF16)
    packed = pltpu.VMEM((n_mb, NZ, rows, width), BF16)
    padded = pltpu.VMEM((n_mb, NZ, NC, CAP, width), BF16)
    pair = pltpu.SemaphoreType.DMA((n_mb, NZ))
    return pl.pallas_call(
        functools.partial(moe_kernel, rows),
        out_shape=jax.ShapeDtypeStruct(tokens.shape, BF16),
        in_specs=[VMEM_SPEC] * 4 + [hbm] * 3,
        out_specs=VMEM_SPEC,
        scratch_shapes=[
            per_mb, pltpu.VMEM((meta.shape[0], n_tok, 2 * n_mb), F32), pltpu.VMEM((2,) + meta.shape, jnp.int32),
            relay, relay, pltpu.VMEM((n_mb, 2, n_tok, width), BF16),
            padded, padded, padded, padded, packed, packed,
            pltpu.VMEM((width, ffn), BF16), pltpu.VMEM((width, ffn), BF16), pltpu.VMEM((ffn, width), BF16),
            pltpu.VMEM((SLOTS, ffn), BF16),
            pltpu.SemaphoreType.DMA((3,)), pltpu.SemaphoreType.DMA((1,)), pltpu.SemaphoreType.DMA((2,)),
            pltpu.SemaphoreType.DMA((n_mb, 3)), pltpu.SemaphoreType.DMA((n_mb, 3)),
            pltpu.SemaphoreType.DMA((n_mb,)), pltpu.SemaphoreType.DMA((n_mb, 2)),
        ] + [pair] * 6,
        compiler_params=pltpu.CompilerParams(
            collective_id=collective_id, has_side_effects=True, vmem_limit_bytes=67_000_000),
        name=f"moe_rows_{rows}",
    )(tokens, meta, prow, gates, w_up1, w_up3, w_down)


def solution(mesh):
    tok_spec = P(None, MESH_AXES, None)
    route_spec = P(None, None, MESH_AXES, None)
    weight_spec = P(None, MESH_AXES, None, None)

    def device_body(tokens_in, expert_ids, gate_vals, w_up1, w_up3, w_down):
        meta, prow, peak = run_route(expert_ids.transpose(0, 1, 3, 2))
        gates = gate_vals.transpose(0, 1, 3, 2)

        def branch(rows, collective_id):
            return lambda: run_moe(rows, collective_id, tokens_in, meta, prow, gates, w_up1, w_up3, w_down)

        return lax.cond(peak[0] <= 176.0, branch(176, 1), branch(SLOTS, 2))

    return jax.shard_map(device_body, mesh=mesh, in_specs=(tok_spec, route_spec, route_spec, weight_spec, weight_spec, weight_spec), out_specs=tok_spec, check_vma=False)
```

```python
import functools

import jax
import jax.numpy as jnp
from jax import lax
from jax.experimental import pallas as pl
from jax.experimental.pallas import tpu as pltpu
from jax.sharding import PartitionSpec as P

ROUTE_SCALE = 2.5
MESH_AXES = ("ez", "ey", "ex")
NZ, NC, CAP = 4, 8, 32
EXPERTS, SLOTS = NZ * NC, NC * CAP
PACKED_ROWS = 176
TILE = 256
BF16, F32 = jnp.bfloat16, jnp.float32
MESH = pl.DeviceIdType.MESH


def dot(lhs, rhs):
    return jnp.dot(lhs, rhs, preferred_element_type=F32)


def dot_t(lhs, rhs):
    return lax.dot_general(lhs, rhs, (((0,), (0,)), ((), ())), preferred_element_type=F32)


def dot_nt(lhs, rhs):
    return lax.dot_general(lhs, rhs, (((1,), (1,)), ((), ())), preferred_element_type=F32)


def one_hot(cond):
    return jnp.where(cond, 1.0, 0.0).astype(BF16)


def iota(shape, dim):
    return lax.broadcasted_iota(jnp.int32, shape, dim)


def place():
    return lax.axis_index("ez"), lax.axis_index("ey") * 4 + lax.axis_index("ex")


def source_of(me_z, k):
    half, far = me_z // 2, k // 2
    near = (1 - k) * me_z + k * (4 * half + 1 - me_z)
    away = (3 - k) * (2 - half) + (k - 2) * (3 - 3 * half)
    return (1 - far) * near + far * away


def plane_id(c):
    return {"ey": c // 4, "ex": c % 4}


def plan_rows(ids_ref, meta_ref, mine):
    n_layers, n_mb, top_k, n_tok = ids_ref.shape
    n_set = n_layers * n_mb
    lanes = n_set * EXPERTS
    expert = iota((EXPERTS, n_tok), 0)
    chosen = [jnp.concatenate([jnp.where(ids_ref[i // n_mb, i % n_mb, j:j + 1, :] == expert, 1.0, 0.0)
                               for i in range(n_set)], axis=0) for j in range(top_k)]
    per_tok = (chosen[0] + chosen[1]).astype(BF16)
    mine[...] = dot_nt(jnp.ones((8, n_tok), BF16), per_tok)
    rank = dot(per_tok, one_hot(iota((n_tok, n_tok), 0) < iota((n_tok, n_tok), 1)))
    totals = dot(per_tok, jnp.ones((n_tok, n_tok), BF16)).astype(BF16)
    row, col = iota((lanes, lanes), 0), iota((lanes, lanes), 1)
    start = dot(one_hot((row // NC == col // NC) & (col < row)), totals)
    which = iota((lanes, n_tok), 0) % EXPERTS
    base = which // NC * SLOTS
    packed = base.astype(F32) + rank + start
    padded = (base + which % NC * CAP).astype(F32) + rank
    for j in range(top_k):
        for i in range(n_set):
            part = slice(i * EXPERTS, (i + 1) * EXPERTS)
            for place_of, at in ((packed, j), (padded, top_k + j)):
                found = jnp.sum(chosen[j][part] * place_of[part], axis=0, keepdims=True)
                meta_ref[i // n_mb, i % n_mb, at:at + 1, :] = found.astype(jnp.int32)


def plan_sources(me_z, me_c, seen, prow_ref, peak_ref):
    n_dev, _, lanes = seen.shape
    n_layers, n_mb = prow_ref.shape[:2]
    row, col = iota((lanes, lanes), 0), iota((lanes, lanes), 1)
    everyone = seen[...].reshape(n_dev * 8, lanes).astype(BF16)
    peak_ref[0] = jnp.max(dot(everyone, one_hot(row // NC == col // NC)))
    sources = jnp.concatenate([seen[source_of(me_z, k) * NC + me_c] for k in range(NZ)], axis=0).astype(BF16)
    lane_of, slot_of = iota((lanes, SLOTS), 0), iota((lanes, SLOTS), 1)
    within = iota((NZ * 8, SLOTS), 1) % CAP
    for i in range(n_layers * n_mb):
        own = lane_of - (i * EXPERTS + me_z * NC)
        amount = dot(sources, one_hot(own == slot_of // CAP)).astype(jnp.int32)
        ahead = dot(sources, one_hot((own >= 0) & (own < slot_of // CAP))).astype(jnp.int32)
        prow_ref[i // n_mb, i % n_mb] = jnp.where(within < amount, ahead + within, -1).reshape(NZ, 8, SLOTS)


def moe_kernel(rows, tok_ref, ids_ref, gate_ref, w1_hbm, w3_hbm, wd_hbm, out_ref, peak_ref,
               meta_ref, prow_ref, mine, seen, ucur, gcol, pmeta, tsend, trecv, tfull, ssend, xrecv, osend, rrecv, ysend, yrecv, w1, w3, wd, hid,
               c_s, c_r, w_sem, m_s, m_r, tz_s, tz_r, tf_s, tf_r, sp_s, sp_r, op_s, op_r, yz_s, yz_r):
    n_layers, n_mb = meta_ref.shape[0], meta_ref.shape[1]
    n_tok, width = ucur.shape[1:]
    ffn = w1.shape[-1]
    me_z, me_c = place()
    source = functools.partial(source_of, me_z)
    near = source(1)
    gateway = source(2)
    inner = (me_z + 1) // 2 % 2
    my_far = 1 - inner

    def peer_c(d):
        return (me_c + d) % NC

    def w_copies(layer):
        return [pltpu.make_async_copy(src.at[layer, 0], dst, w_sem.at[i])
                for i, (src, dst) in enumerate(((w1_hbm, w1), (w3_hbm, w3), (wd_hbm, wd)))]

    def meta_copy(i):
        return pltpu.make_async_remote_copy(
            src_ref=meta_ref, dst_ref=pmeta.at[i], send_sem=m_s.at[0], recv_sem=m_r.at[i],
            device_id={"ez": gateway}, device_id_type=MESH)

    def t_copy(mb, i):
        return pltpu.make_async_remote_copy(
            src_ref=tsend.at[mb, i], dst_ref=trecv.at[mb, i], send_sem=tz_s.at[mb, i], recv_sem=tz_r.at[mb, i],
            device_id={"ez": near}, device_id_type=MESH)

    def full_copy(mb, i):
        return pltpu.make_async_remote_copy(
            src_ref=ucur.at[mb], dst_ref=tfull.at[mb, i], send_sem=tf_s.at[mb], recv_sem=tf_r.at[mb, i],
            device_id={"ez": gateway}, device_id_type=MESH)

    def y_copy(mb, k):
        return pltpu.make_async_remote_copy(
            src_ref=ysend.at[mb, k], dst_ref=yrecv.at[mb, me_z], send_sem=yz_s.at[mb, k], recv_sem=yz_r.at[mb, me_z],
            device_id={"ez": source(k)}, device_id_type=MESH)

    def y_wait(mb, k):
        src = source(k)
        pltpu.make_async_remote_copy(
            src_ref=ysend.at[mb, k], dst_ref=yrecv.at[mb, src], send_sem=yz_s.at[mb, k], recv_sem=yz_r.at[mb, src],
            device_id={"ez": src}, device_id_type=MESH).wait_recv()

    def plane_copy(src, dst, s_sem, r_sem, mb, k, d):
        c = peer_c(d)
        return pltpu.make_async_remote_copy(
            src_ref=src.at[mb, k, c], dst_ref=dst.at[mb, k, me_c], send_sem=s_sem.at[mb, k], recv_sem=r_sem.at[mb, k],
            device_id=plane_id(c), device_id_type=MESH)

    def plane_all(src, dst, s_sem, r_sem, mb, k):
        part = pl.ds(0, NC - 1)
        return pltpu.make_async_remote_copy(
            src_ref=src.at[mb, k, part], dst_ref=dst.at[mb, k, part], send_sem=s_sem.at[mb, k],
            recv_sem=r_sem.at[mb, k], device_id=plane_id(peer_c(1)), device_id_type=MESH)

    def choose(ref, j, n, base):
        row = iota((n, n_tok), 0) + base
        return one_hot((row == ref[j:j + 1, :]) | (row == ref[j + 1:j + 2, :]))

    def send_tokens(layer, mb):
        tsend[mb, 0] = dot(choose(meta_ref.at[layer, mb], 0, rows, near * SLOTS), ucur[mb]).astype(BF16)
        t_copy(mb, 0).start()
        full_copy(mb, my_far).start()

    def packing(layer, mb, k):
        return one_hot(iota((rows, SLOTS), 0) == prow_ref[layer, mb, k, 0:1, :])

    def spread(mb, k, block):
        ssend[mb, k] = block.astype(BF16).reshape(NC, CAP, width)
        for d in range(1, NC):
            plane_copy(ssend, xrecv, sp_s, sp_r, mb, k, d).start()
        xrecv[mb, k, me_c] = ssend[mb, k, me_c]

    def expand_own(layer, mb):
        spread(mb, 0, dot(choose(meta_ref.at[layer, mb], 2, SLOTS, me_z * SLOTS), ucur[mb]))

    def expand(layer, mb, k):
        def from_packed():
            t_copy(mb, k - 1).wait_recv()
            spread(mb, k, dot_t(packing(layer, mb, k), trecv[mb, k - 1]))

        @pl.when((k == 1) | (inner == 0))
        def _():
            from_packed()

        @pl.when((k > 1) & (inner == 1))
        def _():
            i = k - 2
            full_copy(mb, i).wait_recv()
            tsend[mb, k - 1] = dot(choose(pmeta.at[i, layer, mb], 0, rows, near * SLOTS), tfull[mb, i]).astype(BF16)
            t_copy(mb, k - 1).start()
            spread(mb, k, dot(choose(pmeta.at[i, layer, mb], 2, SLOTS, me_z * SLOTS), tfull[mb, i]))

    def expert(mb, k):
        plane_all(ssend, xrecv, sp_s, sp_r, mb, k).wait_recv()

        def up(t, _):
            cols = pl.ds(pl.multiple_of(t * TILE, TILE), TILE)
            x = xrecv[mb, k].reshape(SLOTS, width)
            a = dot(x, w1[:, cols])
            b = dot(x, w3[:, cols])
            hid[:, cols] = (jax.nn.silu(a) * b).astype(BF16)
            return 0

        lax.fori_loop(0, ffn // TILE, up, 0, unroll=True)

        def down(t, _):
            cols = pl.ds(pl.multiple_of(t * TILE, TILE), TILE)
            osend[mb, k, :, :, cols] = dot(hid[...], wd[:, cols]).astype(BF16).reshape(NC, CAP, TILE)
            return 0

        lax.fori_loop(0, width // TILE, down, 0, unroll=True)
        for d in range(1, NC):
            plane_copy(osend, rrecv, op_s, op_r, mb, k, d).start()
        rrecv[mb, k, me_c] = osend[mb, k, me_c]

    def give_back(layer, mb, k):
        plane_all(osend, rrecv, op_s, op_r, mb, k).wait_recv()
        packed = dot(packing(layer, mb, k), rrecv[mb, k].reshape(SLOTS, width)).astype(BF16)

        @pl.when(k == 0)
        def _():
            yrecv[mb, me_z] = packed

        @pl.when(k > 0)
        def _():
            ysend[mb, k] = packed
            y_copy(mb, k).start()

    def combine(layer, mb):
        full_copy(mb, my_far).wait_send()
        for k in (1, 2, 3):
            y_wait(mb, k)
        y = yrecv[mb].reshape(NZ * rows, width)
        shape = (NZ, rows, n_tok)
        row = (iota(shape, 0) * SLOTS + iota(shape, 1)).reshape(NZ * rows, n_tok)
        total = jnp.zeros((n_tok, width), F32)
        for j in range(2):
            picked = dot_t(one_hot(row == meta_ref[layer, mb, j:j + 1, :]), y)
            total = total + gcol[layer, :, 2 * mb + j:2 * mb + j + 1] * picked
        ucur[mb] = (ucur[mb].astype(F32) + ROUTE_SCALE * total).astype(BF16)
        t_copy(mb, 0).wait_send()

        @pl.when(inner == 1)
        def _():
            for i in (1, 2):
                t_copy(mb, i).wait_send()

        for k in range(NZ):
            if k:
                y_copy(mb, k).wait_send()
            plane_all(ssend, xrecv, sp_s, sp_r, mb, k).wait_send()
            plane_all(osend, rrecv, op_s, op_r, mb, k).wait_send()

    n_dev = NZ * NC
    me = me_z * NC + me_c

    def other(d):
        dev = (me + d) % n_dev
        return {"ez": dev // NC, "ey": dev % NC // 4, "ex": dev % 4}

    def count_copy(d):
        return pltpu.make_async_remote_copy(src_ref=mine, dst_ref=seen.at[me], send_sem=c_s, recv_sem=c_r,
                                            device_id=other(d), device_id_type=MESH)

    barrier = pltpu.get_barrier_semaphore()

    def greet(d, _):
        pl.semaphore_signal(barrier, inc=1, device_id=other(d), device_id_type=MESH)
        return 0

    def share(d, _):
        count_copy(d).start()
        return 0

    lax.fori_loop(1, n_dev, greet, 0)
    for copy in w_copies(0):
        copy.start()
    ucur[...] = tok_ref[...]
    plan_rows(ids_ref, meta_ref, mine)
    seen[me] = mine[...]
    pl.semaphore_wait(barrier, n_dev - 1)
    lax.fori_loop(1, n_dev, share, 0)
    meta_copy(my_far).start()
    for mb in range(n_mb):
        send_tokens(0, mb)
        expand_own(0, mb)
    n_gate = 2 * n_mb
    turned = jnp.transpose(gate_ref[...].reshape(n_layers * n_gate, n_tok))
    for layer in range(n_layers):
        gcol[layer] = turned[:, layer * n_gate:(layer + 1) * n_gate]
    rest = pltpu.make_async_remote_copy(
        src_ref=seen.at[pl.ds(0, n_dev - 1)], dst_ref=seen.at[pl.ds(0, n_dev - 1)], send_sem=c_s, recv_sem=c_r,
        device_id=other(1), device_id_type=MESH)
    rest.wait_recv()
    plan_sources(me_z, me_c, seen, prow_ref, peak_ref)
    rest.wait_send()

    @pl.when(inner == 1)
    def _():
        for i in range(2):
            meta_copy(i).wait_recv()

    n_step = n_mb * NZ

    def chunk(j):
        later = (j + 6) // 8
        return later * ((j + 1) // 3 - 1) + (1 - later) * j, later * (1 + (j + 1) % 3)

    def layer_step(layer, _):
        for copy in w_copies(layer):
            copy.wait()

        def step(j, _):
            expert(*chunk(j))

            @pl.when((j == n_step - 1) & (layer + 1 < n_layers))
            def _():
                for copy in w_copies(layer + 1):
                    copy.start()

            @pl.when(j > 0)
            def _():
                give_back(layer, *chunk(j - 1))

            @pl.when(j + 2 < n_step)
            def _():
                expand(layer, *chunk(j + 2))
            return 0

        lax.fori_loop(0, n_step, step, 0)
        give_back(layer, n_mb - 1, NZ - 1)

        for mb in range(n_mb):
            combine(layer, mb)

            @pl.when(layer + 1 < n_layers)
            def _():
                send_tokens(layer + 1, mb)
                expand_own(layer + 1, mb)
        return 0

    lax.fori_loop(0, n_layers, layer_step, 0)
    meta_copy(my_far).wait_send()
    out_ref[...] = ucur[...]


VMEM_SPEC = pl.BlockSpec(memory_space=pltpu.VMEM)


def run_moe(rows, collective_id, tokens, ids, gates, w_up1, w_up3, w_down):
    n_mb, n_tok, width = tokens.shape
    n_layers = ids.shape[0]
    lanes = n_layers * n_mb * EXPERTS
    meta = (n_layers, n_mb, 4, n_tok)
    ffn = w_up1.shape[-1]
    hbm = pl.BlockSpec(memory_space=pl.ANY)
    per_mb = pltpu.VMEM((n_mb, n_tok, width), BF16)
    relay = pltpu.VMEM((n_mb, 3, rows, width), BF16)
    packed = pltpu.VMEM((n_mb, NZ, rows, width), BF16)
    padded = pltpu.VMEM((n_mb, NZ, NC, CAP, width), BF16)
    pair = pltpu.SemaphoreType.DMA((n_mb, NZ))
    return pl.pallas_call(
        functools.partial(moe_kernel, rows),
        out_shape=(jax.ShapeDtypeStruct(tokens.shape, BF16), jax.ShapeDtypeStruct((1,), F32)),
        in_specs=[VMEM_SPEC] * 3 + [hbm] * 3,
        out_specs=(VMEM_SPEC, pl.BlockSpec(memory_space=pltpu.SMEM)),
        scratch_shapes=[
            pltpu.VMEM(meta, jnp.int32), pltpu.VMEM((n_layers, n_mb, NZ, 8, SLOTS), jnp.int32),
            pltpu.VMEM((8, lanes), F32), pltpu.VMEM((EXPERTS, 8, lanes), F32),
            per_mb, pltpu.VMEM((n_layers, n_tok, 2 * n_mb), F32), pltpu.VMEM((2,) + meta, jnp.int32),
            relay, relay, pltpu.VMEM((n_mb, 2, n_tok, width), BF16),
            padded, padded, padded, padded, packed, packed,
            pltpu.VMEM((width, ffn), BF16), pltpu.VMEM((width, ffn), BF16), pltpu.VMEM((ffn, width), BF16),
            pltpu.VMEM((SLOTS, ffn), BF16),
            pltpu.SemaphoreType.DMA, pltpu.SemaphoreType.DMA,
            pltpu.SemaphoreType.DMA((3,)), pltpu.SemaphoreType.DMA((1,)), pltpu.SemaphoreType.DMA((2,)),
            pltpu.SemaphoreType.DMA((n_mb, 3)), pltpu.SemaphoreType.DMA((n_mb, 3)),
            pltpu.SemaphoreType.DMA((n_mb,)), pltpu.SemaphoreType.DMA((n_mb, 2)),
        ] + [pair] * 6,
        compiler_params=pltpu.CompilerParams(
            collective_id=collective_id, has_side_effects=True, vmem_limit_bytes=67_000_000),
        name=f"moe_rows_{rows}",
    )(tokens, ids, gates, w_up1, w_up3, w_down)


def solution(mesh):
    tok_spec = P(None, MESH_AXES, None)
    route_spec = P(None, None, MESH_AXES, None)
    weight_spec = P(None, MESH_AXES, None, None)

    def device_body(tokens_in, expert_ids, gate_vals, w_up1, w_up3, w_down):
        ids = expert_ids.transpose(0, 1, 3, 2)
        gates = gate_vals.transpose(0, 1, 3, 2)
        args = (tokens_in, ids, gates, w_up1, w_up3, w_down)
        out, peak = run_moe(PACKED_ROWS, 1, *args)
        return lax.cond(peak[0] <= PACKED_ROWS, lambda: out, lambda: run_moe(SLOTS, 2, *args)[0])

    return jax.shard_map(device_body, mesh=mesh, in_specs=(tok_spec, route_spec, route_spec, weight_spec, weight_spec, weight_spec), out_specs=tok_spec, check_vma=False)
```

```python
import functools

import jax
import jax.numpy as jnp
from jax import lax
from jax.experimental import pallas as pl
from jax.experimental.pallas import tpu as pltpu
from jax.sharding import PartitionSpec as P

ROUTE_SCALE = 2.5
MESH_AXES = ("ez", "ey", "ex")
NZ, NC, CAP = 4, 8, 32
EXPERTS, SLOTS = NZ * NC, NC * CAP
PACKED_ROWS = 176
PLANE_ORDER = (6, 7, 2, 4, 3, 5, 1)
TILE = 256
BF16, F32 = jnp.bfloat16, jnp.float32
MESH = pl.DeviceIdType.MESH


def dot(lhs, rhs):
    return jnp.dot(lhs, rhs, preferred_element_type=F32)


def dot_t(lhs, rhs):
    return lax.dot_general(lhs, rhs, (((0,), (0,)), ((), ())), preferred_element_type=F32)


def dot_nt(lhs, rhs):
    return lax.dot_general(lhs, rhs, (((1,), (1,)), ((), ())), preferred_element_type=F32)


def one_hot(cond):
    return jnp.where(cond, 1.0, 0.0).astype(BF16)


def iota(shape, dim):
    return lax.broadcasted_iota(jnp.int32, shape, dim)


def place():
    return lax.axis_index("ez"), lax.axis_index("ey") * 4 + lax.axis_index("ex")


def source_of(me_z, k):
    half, far = me_z // 2, k // 2
    near = (1 - k) * me_z + k * (4 * half + 1 - me_z)
    away = (3 - k) * (2 - half) + (k - 2) * (3 - 3 * half)
    return (1 - far) * near + far * away


def plane_id(c):
    return {"ey": c // 4, "ex": c % 4}


def plan_rows(ids_ref, meta_ref, mine):
    n_layers, n_mb, top_k, n_tok = ids_ref.shape
    n_set = n_layers * n_mb
    lanes = n_set * EXPERTS
    expert = iota((EXPERTS, n_tok), 0)
    chosen = [jnp.concatenate([jnp.where(ids_ref[i // n_mb, i % n_mb, j:j + 1, :] == expert, 1.0, 0.0)
                               for i in range(n_set)], axis=0) for j in range(top_k)]
    per_tok = (chosen[0] + chosen[1]).astype(BF16)
    mine[...] = dot_nt(jnp.ones((8, n_tok), BF16), per_tok)
    rank = dot(per_tok, one_hot(iota((n_tok, n_tok), 0) < iota((n_tok, n_tok), 1)))
    totals = dot(per_tok, jnp.ones((n_tok, n_tok), BF16)).astype(BF16)
    row, col = iota((lanes, lanes), 0), iota((lanes, lanes), 1)
    start = dot(one_hot((row // NC == col // NC) & (col < row)), totals)
    which = iota((lanes, n_tok), 0) % EXPERTS
    base = which // NC * SLOTS
    packed = base.astype(F32) + rank + start
    padded = (base + which % NC * CAP).astype(F32) + rank
    for j in range(top_k):
        for i in range(n_set):
            part = slice(i * EXPERTS, (i + 1) * EXPERTS)
            for place_of, at in ((packed, j), (padded, top_k + j)):
                found = jnp.sum(chosen[j][part] * place_of[part], axis=0, keepdims=True)
                meta_ref[i // n_mb, i % n_mb, at:at + 1, :] = found.astype(jnp.int32)


def plan_sources(me_z, me_c, seen, prow_ref, peak_ref):
    n_dev, _, lanes = seen.shape
    n_layers, n_mb = prow_ref.shape[:2]
    row, col = iota((lanes, lanes), 0), iota((lanes, lanes), 1)
    everyone = seen[...].reshape(n_dev * 8, lanes).astype(BF16)
    peak_ref[0] = jnp.max(dot(everyone, one_hot(row // NC == col // NC)))
    sources = jnp.concatenate([seen[source_of(me_z, k) * NC + me_c] for k in range(NZ)], axis=0).astype(BF16)
    lane_of, slot_of = iota((lanes, SLOTS), 0), iota((lanes, SLOTS), 1)
    within = iota((NZ * 8, SLOTS), 1) % CAP
    for i in range(n_layers * n_mb):
        own = lane_of - (i * EXPERTS + me_z * NC)
        amount = dot(sources, one_hot(own == slot_of // CAP)).astype(jnp.int32)
        ahead = dot(sources, one_hot((own >= 0) & (own < slot_of // CAP))).astype(jnp.int32)
        prow_ref[i // n_mb, i % n_mb] = jnp.where(within < amount, ahead + within, -1).reshape(NZ, 8, SLOTS)


def moe_kernel(rows, tok_ref, ids_ref, gate_ref, w1_hbm, w3_hbm, wd_hbm, out_ref, peak_ref,
               meta_ref, prow_ref, mine, seen, ucur, gcol, pmeta, tsend, trecv, tfull, ssend, xrecv, osend, rrecv, ysend, yrecv, w1, w3, wd, hid,
               c_s, c_r, w_sem, m_s, m_r, tz_s, tz_r, tf_s, tf_r, sp_s, sp_r, op_s, op_r, yz_s, yz_r):
    n_layers, n_mb = meta_ref.shape[0], meta_ref.shape[1]
    n_tok, width = ucur.shape[1:]
    ffn = w1.shape[-1]
    me_z, me_c = place()
    source = functools.partial(source_of, me_z)
    near = source(1)
    gateway = source(2)
    inner = (me_z + 1) // 2 % 2
    my_far = 1 - inner

    def peer_c(d):
        return sum(bit * ((me_c // bit + d // bit) % 2) for bit in (1, 2, 4))

    def w_copies(layer):
        return [pltpu.make_async_copy(src.at[layer, 0], dst, w_sem.at[i])
                for i, (src, dst) in enumerate(((w1_hbm, w1), (w3_hbm, w3), (wd_hbm, wd)))]

    def meta_copy(i):
        return pltpu.make_async_remote_copy(
            src_ref=meta_ref, dst_ref=pmeta.at[i], send_sem=m_s.at[0], recv_sem=m_r.at[i],
            device_id={"ez": gateway}, device_id_type=MESH)

    def t_copy(mb, i):
        return pltpu.make_async_remote_copy(
            src_ref=tsend.at[mb, i], dst_ref=trecv.at[mb, i], send_sem=tz_s.at[mb, i], recv_sem=tz_r.at[mb, i],
            device_id={"ez": near}, device_id_type=MESH)

    def full_copy(mb, i):
        return pltpu.make_async_remote_copy(
            src_ref=ucur.at[mb], dst_ref=tfull.at[mb, i], send_sem=tf_s.at[mb], recv_sem=tf_r.at[mb, i],
            device_id={"ez": gateway}, device_id_type=MESH)

    def y_copy(mb, k):
        return pltpu.make_async_remote_copy(
            src_ref=ysend.at[mb, k], dst_ref=yrecv.at[mb, me_z], send_sem=yz_s.at[mb, k], recv_sem=yz_r.at[mb, me_z],
            device_id={"ez": source(k)}, device_id_type=MESH)

    def y_wait(mb, k):
        src = source(k)
        pltpu.make_async_remote_copy(
            src_ref=ysend.at[mb, k], dst_ref=yrecv.at[mb, src], send_sem=yz_s.at[mb, k], recv_sem=yz_r.at[mb, src],
            device_id={"ez": src}, device_id_type=MESH).wait_recv()

    def plane_copy(src, dst, s_sem, r_sem, mb, k, d):
        c = peer_c(d)
        return pltpu.make_async_remote_copy(
            src_ref=src.at[mb, k, c], dst_ref=dst.at[mb, k, me_c], send_sem=s_sem.at[mb, k], recv_sem=r_sem.at[mb, k],
            device_id=plane_id(c), device_id_type=MESH)

    def plane_all(src, dst, s_sem, r_sem, mb, k):
        part = pl.ds(0, NC - 1)
        return pltpu.make_async_remote_copy(
            src_ref=src.at[mb, k, part], dst_ref=dst.at[mb, k, part], send_sem=s_sem.at[mb, k],
            recv_sem=r_sem.at[mb, k], device_id=plane_id(peer_c(1)), device_id_type=MESH)

    def choose(ref, j, n, base):
        row = iota((n, n_tok), 0) + base
        return one_hot((row == ref[j:j + 1, :]) | (row == ref[j + 1:j + 2, :]))

    def send_tokens(layer, mb):
        tsend[mb, 0] = dot(choose(meta_ref.at[layer, mb], 0, rows, near * SLOTS), ucur[mb]).astype(BF16)
        t_copy(mb, 0).start()
        full_copy(mb, my_far).start()

    def packing(layer, mb, k):
        return one_hot(iota((rows, SLOTS), 0) == prow_ref[layer, mb, k, 0:1, :])

    def spread(mb, k, block):
        ssend[mb, k] = block.astype(BF16).reshape(NC, CAP, width)
        for d in PLANE_ORDER:
            plane_copy(ssend, xrecv, sp_s, sp_r, mb, k, d).start()
        xrecv[mb, k, me_c] = ssend[mb, k, me_c]

    def expand_own(layer, mb):
        spread(mb, 0, dot(choose(meta_ref.at[layer, mb], 2, SLOTS, me_z * SLOTS), ucur[mb]))

    def expand(layer, mb, k):
        def from_packed():
            t_copy(mb, k - 1).wait_recv()
            spread(mb, k, dot_t(packing(layer, mb, k), trecv[mb, k - 1]))

        @pl.when((k == 1) | (inner == 0))
        def _():
            from_packed()

        @pl.when((k > 1) & (inner == 1))
        def _():
            i = k - 2
            full_copy(mb, i).wait_recv()
            tsend[mb, k - 1] = dot(choose(pmeta.at[i, layer, mb], 0, rows, near * SLOTS), tfull[mb, i]).astype(BF16)
            t_copy(mb, k - 1).start()
            spread(mb, k, dot(choose(pmeta.at[i, layer, mb], 2, SLOTS, me_z * SLOTS), tfull[mb, i]))

    def expert(mb, k):
        plane_all(ssend, xrecv, sp_s, sp_r, mb, k).wait_recv()

        def up(t, _):
            cols = pl.ds(pl.multiple_of(t * TILE, TILE), TILE)
            x = xrecv[mb, k].reshape(SLOTS, width)
            a = dot(x, w1[:, cols])
            b = dot(x, w3[:, cols])
            hid[:, cols] = (jax.nn.silu(a) * b).astype(BF16)
            return 0

        lax.fori_loop(0, ffn // TILE, up, 0, unroll=True)

        def down(t, _):
            cols = pl.ds(pl.multiple_of(t * TILE, TILE), TILE)
            osend[mb, k, :, :, cols] = dot(hid[...], wd[:, cols]).astype(BF16).reshape(NC, CAP, TILE)
            return 0

        lax.fori_loop(0, width // TILE, down, 0, unroll=True)
        for d in PLANE_ORDER:
            plane_copy(osend, rrecv, op_s, op_r, mb, k, d).start()
        rrecv[mb, k, me_c] = osend[mb, k, me_c]

    def give_back(layer, mb, k):
        plane_all(osend, rrecv, op_s, op_r, mb, k).wait_recv()
        packed = dot(packing(layer, mb, k), rrecv[mb, k].reshape(SLOTS, width)).astype(BF16)

        @pl.when(k == 0)
        def _():
            yrecv[mb, me_z] = packed

        @pl.when(k > 0)
        def _():
            ysend[mb, k] = packed
            y_copy(mb, k).start()

    def combine(layer, mb):
        full_copy(mb, my_far).wait_send()
        for k in (1, 2, 3):
            y_wait(mb, k)
        y = yrecv[mb].reshape(NZ * rows, width)
        shape = (NZ, rows, n_tok)
        row = (iota(shape, 0) * SLOTS + iota(shape, 1)).reshape(NZ * rows, n_tok)
        total = jnp.zeros((n_tok, width), F32)
        for j in range(2):
            picked = dot_t(one_hot(row == meta_ref[layer, mb, j:j + 1, :]), y)
            total = total + gcol[layer, :, 2 * mb + j:2 * mb + j + 1] * picked
        ucur[mb] = (ucur[mb].astype(F32) + ROUTE_SCALE * total).astype(BF16)
        t_copy(mb, 0).wait_send()

        @pl.when(inner == 1)
        def _():
            for i in (1, 2):
                t_copy(mb, i).wait_send()

        for k in range(NZ):
            if k:
                y_copy(mb, k).wait_send()
            plane_all(ssend, xrecv, sp_s, sp_r, mb, k).wait_send()
            plane_all(osend, rrecv, op_s, op_r, mb, k).wait_send()

    n_dev = NZ * NC
    me = me_z * NC + me_c

    def other(d):
        dev = (me + d) % n_dev
        return {"ez": dev // NC, "ey": dev % NC // 4, "ex": dev % 4}

    def count_copy(d):
        return pltpu.make_async_remote_copy(src_ref=mine, dst_ref=seen.at[me], send_sem=c_s, recv_sem=c_r,
                                            device_id=other(d), device_id_type=MESH)

    barrier = pltpu.get_barrier_semaphore()

    def greet(d, _):
        pl.semaphore_signal(barrier, inc=1, device_id=other(d), device_id_type=MESH)
        return 0

    def share(d, _):
        count_copy(d).start()
        return 0

    lax.fori_loop(1, n_dev, greet, 0)
    for copy in w_copies(0):
        copy.start()
    ucur[...] = tok_ref[...]
    plan_rows(ids_ref, meta_ref, mine)
    seen[me] = mine[...]
    pl.semaphore_wait(barrier, n_dev - 1)
    lax.fori_loop(1, n_dev, share, 0)
    meta_copy(my_far).start()
    for mb in range(n_mb):
        send_tokens(0, mb)
        expand_own(0, mb)
    n_gate = 2 * n_mb
    turned = jnp.transpose(gate_ref[...].reshape(n_layers * n_gate, n_tok))
    for layer in range(n_layers):
        gcol[layer] = turned[:, layer * n_gate:(layer + 1) * n_gate]
    rest = pltpu.make_async_remote_copy(
        src_ref=seen.at[pl.ds(0, n_dev - 1)], dst_ref=seen.at[pl.ds(0, n_dev - 1)], send_sem=c_s, recv_sem=c_r,
        device_id=other(1), device_id_type=MESH)
    rest.wait_recv()
    plan_sources(me_z, me_c, seen, prow_ref, peak_ref)
    rest.wait_send()

    @pl.when(inner == 1)
    def _():
        for i in range(2):
            meta_copy(i).wait_recv()

    n_step = n_mb * NZ

    def chunk(j):
        later = (j + 6) // 8
        return later * ((j + 1) // 3 - 1) + (1 - later) * j, later * (1 + (j + 1) % 3)

    def layer_step(layer, _):
        for copy in w_copies(layer):
            copy.wait()

        def step(j, _):
            expert(*chunk(j))

            @pl.when((j == n_step - 1) & (layer + 1 < n_layers))
            def _():
                for copy in w_copies(layer + 1):
                    copy.start()

            @pl.when(j > 0)
            def _():
                give_back(layer, *chunk(j - 1))

            @pl.when(j + 2 < n_step)
            def _():
                expand(layer, *chunk(j + 2))
            return 0

        lax.fori_loop(0, n_step, step, 0)
        give_back(layer, n_mb - 1, NZ - 1)

        for mb in range(n_mb):
            combine(layer, mb)

            @pl.when(layer + 1 < n_layers)
            def _():
                send_tokens(layer + 1, mb)
                expand_own(layer + 1, mb)
        return 0

    lax.fori_loop(0, n_layers, layer_step, 0)
    meta_copy(my_far).wait_send()
    out_ref[...] = ucur[...]


VMEM_SPEC = pl.BlockSpec(memory_space=pltpu.VMEM)


def run_moe(rows, collective_id, tokens, ids, gates, w_up1, w_up3, w_down):
    n_mb, n_tok, width = tokens.shape
    n_layers = ids.shape[0]
    lanes = n_layers * n_mb * EXPERTS
    meta = (n_layers, n_mb, 4, n_tok)
    ffn = w_up1.shape[-1]
    hbm = pl.BlockSpec(memory_space=pl.ANY)
    per_mb = pltpu.VMEM((n_mb, n_tok, width), BF16)
    relay = pltpu.VMEM((n_mb, 3, rows, width), BF16)
    packed = pltpu.VMEM((n_mb, NZ, rows, width), BF16)
    padded = pltpu.VMEM((n_mb, NZ, NC, CAP, width), BF16)
    pair = pltpu.SemaphoreType.DMA((n_mb, NZ))
    return pl.pallas_call(
        functools.partial(moe_kernel, rows),
        out_shape=(jax.ShapeDtypeStruct(tokens.shape, BF16), jax.ShapeDtypeStruct((1,), F32)),
        in_specs=[VMEM_SPEC] * 3 + [hbm] * 3,
        out_specs=(VMEM_SPEC, pl.BlockSpec(memory_space=pltpu.SMEM)),
        scratch_shapes=[
            pltpu.VMEM(meta, jnp.int32), pltpu.VMEM((n_layers, n_mb, NZ, 8, SLOTS), jnp.int32),
            pltpu.VMEM((8, lanes), F32), pltpu.VMEM((EXPERTS, 8, lanes), F32),
            per_mb, pltpu.VMEM((n_layers, n_tok, 2 * n_mb), F32), pltpu.VMEM((2,) + meta, jnp.int32),
            relay, relay, pltpu.VMEM((n_mb, 2, n_tok, width), BF16),
            padded, padded, padded, padded, packed, packed,
            pltpu.VMEM((width, ffn), BF16), pltpu.VMEM((width, ffn), BF16), pltpu.VMEM((ffn, width), BF16),
            pltpu.VMEM((SLOTS, ffn), BF16),
            pltpu.SemaphoreType.DMA, pltpu.SemaphoreType.DMA,
            pltpu.SemaphoreType.DMA((3,)), pltpu.SemaphoreType.DMA((1,)), pltpu.SemaphoreType.DMA((2,)),
            pltpu.SemaphoreType.DMA((n_mb, 3)), pltpu.SemaphoreType.DMA((n_mb, 3)),
            pltpu.SemaphoreType.DMA((n_mb,)), pltpu.SemaphoreType.DMA((n_mb, 2)),
        ] + [pair] * 6,
        compiler_params=pltpu.CompilerParams(
            collective_id=collective_id, has_side_effects=True, vmem_limit_bytes=67_000_000),
        name=f"moe_rows_{rows}",
    )(tokens, ids, gates, w_up1, w_up3, w_down)


def solution(mesh):
    tok_spec = P(None, MESH_AXES, None)
    route_spec = P(None, None, MESH_AXES, None)
    weight_spec = P(None, MESH_AXES, None, None)

    def device_body(tokens_in, expert_ids, gate_vals, w_up1, w_up3, w_down):
        ids = expert_ids.transpose(0, 1, 3, 2)
        gates = gate_vals.transpose(0, 1, 3, 2)
        args = (tokens_in, ids, gates, w_up1, w_up3, w_down)
        out, peak = run_moe(PACKED_ROWS, 1, *args)
        return lax.cond(peak[0] <= PACKED_ROWS, lambda: out, lambda: run_moe(SLOTS, 2, *args)[0])

    return jax.shard_map(device_body, mesh=mesh, in_specs=(tok_spec, route_spec, route_spec, weight_spec, weight_spec, weight_spec), out_specs=tok_spec, check_vma=False)
```
